32 devices in a mesh: gy: 4 (over x, core), gx: 8 (over z, y).
Axes of the slice: x: 2, y: 2, z: 4, core: 2. Of those that a mesh axis runs over, the one named last changes fastest.
Arguments:
- model_field: float32 [60, 1024, 1024], P(None, 'gy', 'gx'), may hold values from -160 to 160
- driver_field: float32 [60, 1024, 1024], P(None, 'gy', 'gx'), may hold values from -60 to 60
- nudge_rate: float32 [60], replicated, may hold values from 0.1 to 0.5
- increment_cap: float32 [60], replicated, may hold values from 1 to 3
Outputs:
- nudged: float32 [60, 1024, 1024], P(None, 'gy', 'gx')
The draws below stay inside these ranges and needn't reach their ends.
All inputs are finite; a program needn't handle non-finite values.
Results may differ from the reference program's by a relative error of at most 0.00005.
Values sent between devices are 32-bit elements; how exact they have to be, the bound alone decides.
A program may use at most 64 MiB of HBM per device.

```python
import math
import jax
import jax.numpy as jnp
from jax import lax

MODES = 24
FIELDS = 60
NY = 1024
NX = 1024


def driver_table(length_all):
    positions = lax.iota(jnp.int32, length_all)
    wavenumber = jnp.concatenate([lax.iota(jnp.int32, 32), lax.iota(jnp.int32, 32) + 1])
    phases = positions[:, None] * wavenumber[None, :] % length_all
    angles = phases.astype(jnp.float32) * (2.0 * math.pi / length_all)
    column = lax.iota(jnp.int32, 64)
    return jnp.where(column[None, :] < 32, jnp.cos(angles), jnp.sin(angles))


def field_amplitude(key):
    order_key, offset_key = jax.random.split(jax.random.fold_in(key, 97), 2)
    order = jax.random.permutation(order_key, FIELDS).astype(jnp.float32)
    offset = jax.random.uniform(offset_key, (FIELDS,), jnp.float32, 0.0, 1.0)
    logs = math.log(0.05) + (order + offset) / FIELDS * math.log(40.0)
    return jnp.exp(logs)


def draw_model_field(key, part):
    first, second, third = jax.random.split(jax.random.fold_in(key, 11), 3)
    amplitude = field_amplitude(key)[:, None, None]
    growth = 0.5 * math.log(3.0)
    noise = jnp.clip(jax.random.normal(first, (FIELDS, NY, NX), jnp.float32), -5.0, 5.0)
    trend_rows = jnp.exp(growth * lax.iota(jnp.int32, NY).astype(jnp.float32) / NY)
    trend_columns = jnp.exp(growth * lax.iota(jnp.int32, NX).astype(jnp.float32) / NX)
    scale_rows = jnp.exp(jax.random.uniform(second, (NY,), jnp.float32, 0.0, 0.5 * math.log(10.0)))
    scale_columns = jnp.exp(jax.random.uniform(third, (NX,), jnp.float32, 0.0, 0.5 * math.log(10.0)))
    rows_factor = (trend_rows * scale_rows)[None, :, None]
    columns_factor = (trend_columns * scale_columns)[None, None, :]
    return 0.5 * noise * rows_factor * columns_factor * amplitude


def draw_driver_field(key, part):
    first, second = jax.random.split(jax.random.fold_in(key, 23), 2)
    amplitude = field_amplitude(key)[:, None, None]
    highest = lax.Precision.HIGHEST
    weights = jax.random.normal(first, (FIELDS, 64, 64), jnp.float32) * (3.0 / 32.0)
    table_rows = driver_table(NY)
    table_columns = driver_table(NX)
    rows_part = jnp.einsum('yj,fjk->fyk', table_rows, weights, precision=highest)
    smooth = jnp.einsum('fyk,xk->fyx', rows_part, table_columns, precision=highest)
    smooth = jnp.clip(smooth, -25.0, 25.0)
    rough = jnp.clip(jax.random.normal(second, (FIELDS, NY, NX), jnp.float32), -5.0, 5.0)
    return (smooth + 0.2 * rough) * amplitude


def setup_inputs(seed: int = 0) -> dict:
    keys = jax.random.split(jax.random.key(seed), 5)
    return {
        "model_field": draw_model_field(jax.random.fold_in(keys[4], 71), 0),
        "driver_field": draw_driver_field(jax.random.fold_in(keys[4], 71), 0),
        "nudge_rate": jnp.clip(jnp.exp(jax.random.uniform(keys[2], (FIELDS,), jnp.float32, math.log(0.1), math.log(0.5))), 0.1, 0.5),
        "increment_cap": jnp.clip(jnp.exp(jax.random.uniform(keys[3], (FIELDS,), jnp.float32, math.log(1.0), math.log(3.0))), 1.0, 3.0),
    }


epsilon = 1e-06

def basis_table(cell_count, start, length_all):
    positions = start + lax.iota(jnp.int32, cell_count)
    wavenumber = jnp.concatenate([lax.iota(jnp.int32, MODES), lax.iota(jnp.int32, MODES) + 1])
    phases = positions[:, None] * wavenumber[None, :] % length_all
    angles = phases.astype(jnp.float32) * (2.0 * math.pi / length_all)
    column = lax.iota(jnp.int32, 2 * MODES)
    weights = jnp.where(column == 0, math.sqrt(1.0 / length_all), math.sqrt(2.0 / length_all))
    return jnp.where(column[None, :] < MODES, jnp.cos(angles), jnp.sin(angles)) * weights[None, :]

def reference(model_field, driver_field, nudge_rate, increment_cap):
    highest = lax.Precision.HIGHEST
    basis_rows = basis_table(NY, 0, NY)
    basis_columns = basis_table(NX, 0, NX)

    def analyse(field_pair):
        model_slab, driver_slab = field_pair
        difference = driver_slab - model_slab
        along_x = jnp.dot(difference, basis_columns, precision=highest)
        coefficient = jnp.dot(basis_rows.T, along_x, precision=highest)
        return (jnp.sum(difference * difference), coefficient)
    squares, coefficients = lax.map(analyse, (model_field, driver_field))
    spread = jnp.sqrt(squares / (NY * NX) + epsilon)
    strength = nudge_rate * jnp.minimum(1.0, increment_cap / spread)

    def build(entries):
        model_slab, coefficient, strength_one = entries
        rows_part = jnp.dot(basis_rows, coefficient, precision=highest)
        large_scale = jnp.dot(rows_part, basis_columns.T, precision=highest)
        return model_slab + strength_one * large_scale
    return lax.map(build, (model_field, coefficients, strength))
```

```python
import functools
import math

import jax
import jax.numpy as jnp
import numpy as np
from jax import lax
from jax.experimental import pallas as pl
from jax.experimental.pallas import tpu as pltpu
from jax.sharding import PartitionSpec as P

MODES = 24
KEPT = 2 * MODES
HALF = 64
LANES = 2 * HALF
EPSILON = 1e-06
FIELDS_STEP = 4
SLOTS_CHUNK = 2
MESH = pl.DeviceIdType.MESH
F32, BF16 = jnp.float32, jnp.bfloat16


def split(value):
    high = value.astype(BF16)
    return high, (value - high.astype(F32)).astype(BF16)


def dot(a, b):
    return jnp.dot(a, b, preferred_element_type=F32)


def basis_table(length):
    position = np.arange(length)[:, None]
    number = np.concatenate([np.arange(MODES), np.arange(MODES) + 1])[None, :]
    angle = (position * number % length) * (2.0 * math.pi / length)
    column = np.arange(KEPT)[None, :]
    weight = np.where(column == 0, math.sqrt(1.0 / length), math.sqrt(2.0 / length))
    table = (np.where(column < MODES, np.cos(angle), np.sin(angle)) * weight).astype(np.float32)
    high = table.astype(BF16)
    return high, (table - high.astype(np.float32)).astype(BF16)


def tables(row_total, column_total, ny, nx):
    rows, columns = row_total // ny, column_total // nx
    yh, yl = (part.reshape(ny, rows, KEPT) for part in basis_table(row_total))
    xh, xl = (part.reshape(nx, columns, KEPT) for part in basis_table(column_total))
    gap = np.zeros((nx, columns, HALF - KEPT), BF16)
    twice = [np.concatenate([part, gap, part, gap], axis=2) for part in (xh, xl)]
    x_in = np.stack(twice, axis=1)
    x_out = np.ascontiguousarray(np.swapaxes(x_in, 2, 3))
    y_in = np.ascontiguousarray(np.swapaxes(np.concatenate([yh, yl], axis=2), 1, 2))
    y_out = np.concatenate([yh, yh, yl], axis=2)
    return y_in, x_in, y_out, x_out


def owner_x(slot, nx):
    return (slot % SLOTS_CHUNK) * (nx // SLOTS_CHUNK) + slot // SLOTS_CHUNK


def analysis_kernel(
    ny, nx, cells,
    model, driver, y_table, x_table, rate, cap, full,
    model_v, driver_v, y_v, x_v, weight, coef, from_y, row_sum, from_x,
    in_sem, table_sem, send_y, recv_y, send_x, recv_x,
    gather_x_send, gather_x_recv, gather_y_send, gather_y_recv, core_send, core_recv,
):
    fields, rows, columns = model.shape
    my_y, my_x = lax.axis_index("gy"), lax.axis_index("gx")
    pairs, steps = fields // 2, fields // FIELDS_STEP
    chunk_pairs = SLOTS_CHUNK * ny
    chunk_steps = chunk_pairs // 2
    chunks = nx // SLOTS_CHUNK

    def load(step):
        part = pl.ds(step * FIELDS_STEP, FIELDS_STEP)
        return (
            pltpu.make_async_copy(model.at[part], model_v.at[part], in_sem.at[step, 0]),
            pltpu.make_async_copy(driver.at[part], driver_v.at[part], in_sem.at[step, 1]),
        )

    table_copies = (
        pltpu.make_async_copy(y_table.at[my_y], y_v, table_sem.at[0]),
        pltpu.make_async_copy(x_table.at[my_x], x_v, table_sem.at[1]),
    )
    for copy in table_copies:
        copy.start()

    @pl.loop(0, steps)
    def _(step):
        for copy in load(step):
            copy.start()

    barrier = pltpu.get_barrier_semaphore()
    for k in range(1, ny):
        pl.semaphore_signal(
            barrier, inc=1, device_id=(lax.rem(my_y + k, ny), my_x), device_id_type=MESH
        )
    for k in range(1, nx):
        pl.semaphore_signal(
            barrier, inc=1, device_id=(my_y, lax.rem(my_x + k, nx)), device_id_type=MESH
        )

    for pair in range(pairs, ny * nx):
        coef[pair % ny, pair // ny] = jnp.zeros((KEPT, LANES), F32)
    for copy in table_copies:
        copy.wait()
    lane_w = lax.broadcasted_iota(jnp.int32, (columns, LANES), 1)
    for part, order in ((0, (0, 2)), (1, (1,))):
        value = x_v[part].astype(F32)
        left = jnp.where(lane_w < HALF, value, 0.0).astype(BF16)
        right = jnp.where(lane_w < HALF, 0.0, value).astype(BF16)
        for at in ((0, 1), (2,))[part]:
            weight[pl.ds(at * columns, columns)] = left
            weight[pl.ds((3 + at) * columns, columns)] = right

    lane = lax.broadcasted_iota(jnp.int32, (8, LANES), 1)

    def compute(step):
        for copy in load(step):
            copy.wait()
        sums, squares = [], []
        for pair in range(FIELDS_STEP // 2):
            blocks, marks = [], jnp.zeros((8, LANES), F32)
            for field in range(2):
                at = step * FIELDS_STEP + pair * 2 + field
                difference = driver_v[at] - model_v[at]
                high, low = split(difference)
                blocks += [high, low, high]
                part = jnp.sum((difference * difference).reshape(rows // 8, 8, columns), axis=0)
                mark = jnp.sum(part, axis=1, keepdims=True)
                marks = jnp.where(lane == field * HALF + KEPT, mark, marks)
            sums.append(dot(jnp.concatenate(blocks, axis=1), weight[...]))
            squares.append(marks)
        high, low = split(jnp.concatenate(sums, axis=1))
        first = dot(y_v[...], high)
        found = first[:KEPT] + first[KEPT:] + dot(y_v[:KEPT], low)
        for pair in range(FIELDS_STEP // 2):
            at = step * (FIELDS_STEP // 2) + pair
            g, q = lax.rem(at, ny), lax.div(at, ny)
            block = found[:, pair * LANES:(pair + 1) * LANES]
            coef[g, q, 0:8] = block[0:8] + squares[pair]
            coef[g, q, 8:KEPT] = block[8:]

    def to_rows(chunk, k):
        part = pl.ds(chunk * SLOTS_CHUNK, SLOTS_CHUNK)
        target = lax.rem(my_y + k, ny)
        return pltpu.make_async_remote_copy(
            src_ref=coef.at[target, part], dst_ref=from_y.at[k - 1, part],
            send_sem=send_y.at[chunk, k - 1], recv_sem=recv_y.at[chunk, k - 1],
            device_id=(target, my_x), device_id_type=MESH,
        )

    def to_owner(slot):
        target = owner_x(slot, nx)
        offset = lax.rem(my_x - target + nx, nx)
        return pltpu.make_async_remote_copy(
            src_ref=row_sum.at[slot], dst_ref=from_x.at[offset],
            send_sem=send_x.at[slot], recv_sem=recv_x.at[offset],
            device_id=(my_y, target), device_id_type=MESH,
        )

    def finish(chunk):
        for k in range(1, ny):
            to_rows(chunk, k).wait_recv()
        for slot in range(chunk * SLOTS_CHUNK, (chunk + 1) * SLOTS_CHUNK):
            total = coef[my_y, slot]
            for k in range(1, ny):
                total += from_y[k - 1, slot]
            row_sum[slot] = total

            @pl.when(my_x != owner_x(slot, nx))
            def _():
                to_owner(slot).start()

    for chunk in range(chunks):
        low, high = (min(steps, part * chunk_steps) for part in (chunk, chunk + 1))
        if high > low:
            pl.loop(low, high)(compute)
        if chunk == 0:
            pl.semaphore_wait(barrier, ny + nx - 2)
        for k in range(1, ny):
            to_rows(chunk, k).start()
        if chunk > 0:
            finish(chunk - 1)
    finish(chunks - 1)

    my_slot = lax.rem(my_x, nx // SLOTS_CHUNK) * SLOTS_CHUNK + lax.div(my_x, nx // SLOTS_CHUNK)
    my_pair = my_slot * ny + my_y
    total = row_sum[my_slot]
    for k in range(1, nx):
        pltpu.make_async_remote_copy(
            src_ref=row_sum.at[0], dst_ref=from_x.at[k],
            send_sem=send_x.at[0], recv_sem=recv_x.at[k],
            device_id=(my_y, lax.rem(my_x + k, nx)), device_id_type=MESH,
        ).wait_recv()
        total += from_x[k]
    lane_c = lax.broadcasted_iota(jnp.int32, (KEPT, LANES), 1)
    strength = []
    for field in range(2):
        at = jnp.minimum(my_pair * 2 + field, fields - 1)
        mark = jnp.where(lane_c == field * HALF + KEPT, total, 0.0)
        square = jnp.sum(jnp.sum(mark, axis=0, keepdims=True), axis=1, keepdims=True)
        spread = jnp.sqrt(square / cells + EPSILON)
        strength.append(rate[at] * jnp.minimum(1.0, cap[at] / spread))
    scale = jnp.where(lane_c < HALF, strength[0], strength[1])
    full[my_y, my_x] = jnp.where(lane_c % HALF < KEPT, total * scale, 0.0)

    half_y = ny // 2
    partner = my_y + 1 - 2 * lax.rem(my_y, 2)

    def x_of(k):
        return lax.rem(my_x - k + nx, nx)

    def y_of(j):
        return lax.rem(my_y - 2 * j + ny, ny)

    def gather_x(k):
        return pltpu.make_async_remote_copy(
            src_ref=full.at[my_y, my_x], dst_ref=full.at[my_y, my_x],
            send_sem=gather_x_send.at[k], recv_sem=gather_x_recv.at[k],
            device_id=(my_y, lax.rem(my_x + k, nx)), device_id_type=MESH,
        )

    def gather_y(j, k):
        return pltpu.make_async_remote_copy(
            src_ref=full.at[my_y, x_of(k)], dst_ref=full.at[my_y, x_of(k)],
            send_sem=gather_y_send.at[j, k], recv_sem=gather_y_recv.at[j, k],
            device_id=(lax.rem(my_y + 2 * j, ny), my_x), device_id_type=MESH,
        )

    def to_core(j, k):
        return pltpu.make_async_remote_copy(
            src_ref=full.at[y_of(j), x_of(k)], dst_ref=full.at[y_of(j), x_of(k)],
            send_sem=core_send.at[j, k], recv_sem=core_recv.at[j, k],
            device_id=(partner, my_x), device_id_type=MESH,
        )

    for k in range(1, nx):
        gather_x(k).start()
    for k in range(nx):
        if k:
            gather_x(k).wait_recv()
        for j in range(1, half_y):
            gather_y(j, k).start()
        to_core(0, k).start()
    for k in range(nx):
        for j in range(1, half_y):
            gather_y(j, k).wait_recv()
            to_core(j, k).start()
    for k in range(nx):
        for j in range(half_y):
            to_core(j, k).wait_recv()

    for chunk in range(chunks):
        for k in range(1, ny):
            to_rows(chunk, k).wait_send()
    for slot in range(nx):
        @pl.when(my_x != owner_x(slot, nx))
        def _():
            to_owner(slot).wait_send()
    for k in range(nx):
        if k:
            gather_x(k).wait_send()
        for j in range(half_y):
            if j:
                gather_y(j, k).wait_send()
            to_core(j, k).wait_send()


def build_kernel(ny, nx, model, full, y_table, x_table, out, y_v, x_v, weight, table_sem):
    step = pl.program_id(0)
    columns = model.shape[2]

    @pl.when(step == 0)
    def _():
        copies = (
            pltpu.make_async_copy(y_table.at[lax.axis_index("gy")], y_v, table_sem.at[0]),
            pltpu.make_async_copy(x_table.at[lax.axis_index("gx")], x_v, table_sem.at[1]),
        )
        for copy in copies:
            copy.start()
        for copy in copies:
            copy.wait()
        row = lax.broadcasted_iota(jnp.int32, (LANES, columns), 0)
        for part in range(2):
            value = x_v[part].astype(F32)
            left = jnp.where(row < HALF, value, 0.0).astype(BF16)
            right = jnp.where(row < HALF, 0.0, value).astype(BF16)
            both = jnp.concatenate([left, right], axis=1)
            for at in ((0, 1), (2,))[part]:
                weight[pl.ds(at * LANES, LANES)] = both

    for pair in range(FIELDS_STEP // 2):
        at = step * (FIELDS_STEP // 2) + pair
        high, low = split(full[lax.rem(at, ny), owner_x(lax.div(at, ny), nx)])
        along = dot(y_v[...], jnp.concatenate([high, low, high], axis=0))
        high, low = split(along)
        large = dot(jnp.concatenate([high, low, high], axis=1), weight[...])
        out[2 * pair] = model[2 * pair] + large[:, :columns]
        out[2 * pair + 1] = model[2 * pair + 1] + large[:, columns:]


def per_device(ny, nx, model, driver, rate, cap):
    fields, rows, columns = model.shape
    assert fields % FIELDS_STEP == 0 and fields // 2 <= ny * nx
    assert ny % 2 == 0 and nx % SLOTS_CHUNK == 0
    row_total, column_total = rows * ny, columns * nx
    y_in, x_in, y_out, x_out = (
        jnp.asarray(table) for table in tables(row_total, column_total, ny, nx)
    )
    anywhere = pl.BlockSpec(memory_space=pl.ANY)
    scalars = pl.BlockSpec(memory_space=pltpu.SMEM)
    vector = pl.BlockSpec(memory_space=pltpu.VMEM)
    dma = pltpu.SemaphoreType.DMA
    chunks, half_y = nx // SLOTS_CHUNK, ny // 2
    full = pl.pallas_call(
        functools.partial(analysis_kernel, ny, nx, float(row_total * column_total)),
        out_shape=jax.ShapeDtypeStruct((ny, nx, KEPT, LANES), F32),
        in_specs=[anywhere, anywhere, anywhere, anywhere, scalars, scalars],
        out_specs=vector,
        scratch_shapes=[
            pltpu.VMEM((fields, rows, columns), F32),
            pltpu.VMEM((fields, rows, columns), F32),
            pltpu.VMEM((2 * KEPT, rows), BF16),
            pltpu.VMEM((2, columns, LANES), BF16),
            pltpu.VMEM((6 * columns, LANES), BF16),
            pltpu.VMEM((ny, nx, KEPT, LANES), F32),
            pltpu.VMEM((ny - 1, nx, KEPT, LANES), F32),
            pltpu.VMEM((nx, KEPT, LANES), F32),
            pltpu.VMEM((nx, KEPT, LANES), F32),
            dma((fields // FIELDS_STEP, 2)), dma((2,)),
            dma((chunks, ny - 1)), dma((chunks, ny - 1)), dma((nx,)), dma((nx,)),
            dma((nx,)), dma((nx,)), dma((half_y, nx)), dma((half_y, nx)),
            dma((half_y, nx)), dma((half_y, nx)),
        ],
        compiler_params=pltpu.CompilerParams(
            collective_id=0, has_side_effects=True, vmem_limit_bytes=60 * 2**20
        ),
        name="analysis",
    )(model, driver, y_in, x_in, rate, cap)
    block = pl.BlockSpec((FIELDS_STEP, rows, columns), lambda i: (i, 0, 0))
    return pl.pallas_call(
        functools.partial(build_kernel, ny, nx),
        grid=(fields // FIELDS_STEP,),
        out_shape=jax.ShapeDtypeStruct(model.shape, F32),
        in_specs=[block, vector, anywhere, anywhere],
        out_specs=block,
        scratch_shapes=[
            pltpu.VMEM((rows, 3 * KEPT), BF16),
            pltpu.VMEM((2, LANES, columns), BF16),
            pltpu.VMEM((3 * LANES, 2 * columns), BF16),
            dma((2,)),
        ],
        compiler_params=pltpu.CompilerParams(
            dimension_semantics=("arbitrary",), vmem_limit_bytes=60 * 2**20
        ),
        name="build",
    )(model, full, y_out, x_out)


def solution(mesh):
    return jax.shard_map(
        functools.partial(per_device, mesh.shape["gy"], mesh.shape["gx"]),
        mesh=mesh,
        in_specs=(P(None, "gy", "gx"), P(None, "gy", "gx"), P(), P()),
        out_specs=P(None, "gy", "gx"),
        check_vma=False,
    )
```

```python
import functools
import math

import jax
import jax.numpy as jnp
import numpy as np
from jax import lax
from jax.experimental import pallas as pl
from jax.experimental.pallas import tpu as pltpu
from jax.sharding import PartitionSpec as P

MODES = 24
KEPT = 2 * MODES
HALF = 64
LANES = 2 * HALF
EPSILON = 1e-06
FIELDS_STEP = 4
BUILD_STEP = 12
SLOTS_CHUNK = 2
VMEM_BYTES = 67_043_328
VMEM_SPARE = 2**16
MESH = pl.DeviceIdType.MESH
F32, BF16 = jnp.float32, jnp.bfloat16


def split(value):
    high = value.astype(BF16)
    return high, (value - high.astype(F32)).astype(BF16)


def dot(a, b):
    return jnp.dot(a, b, preferred_element_type=F32)


def basis_table(length):
    position = np.arange(length)[:, None]
    number = np.concatenate([np.arange(MODES), np.arange(MODES) + 1])[None, :]
    angle = (position * number % length) * (2.0 * math.pi / length)
    column = np.arange(KEPT)[None, :]
    weight = np.where(column == 0, math.sqrt(1.0 / length), math.sqrt(2.0 / length))
    table = (np.where(column < MODES, np.cos(angle), np.sin(angle)) * weight).astype(np.float32)
    high = table.astype(BF16)
    return high, (table - high.astype(np.float32)).astype(BF16)


def tables(row_total, column_total, ny, nx):
    rows, columns = row_total // ny, column_total // nx
    yh, yl = (part.reshape(ny, rows, KEPT) for part in basis_table(row_total))
    xh, xl = (part.reshape(nx, columns, KEPT) for part in basis_table(column_total))
    gap = np.zeros((nx, columns, HALF - KEPT), BF16)
    twice = [np.concatenate([part, gap, part, gap], axis=2) for part in (xh, xl)]
    x_in = np.stack(twice, axis=1)
    x_out = np.ascontiguousarray(np.swapaxes(x_in, 2, 3))
    y_in = np.ascontiguousarray(np.swapaxes(np.concatenate([yh, yl], axis=2), 1, 2))
    y_out = np.concatenate([yh, yh, yl], axis=2)
    return y_in, x_in, y_out, x_out


def owner_x(slot, nx):
    return (slot % SLOTS_CHUNK) * (nx // SLOTS_CHUNK) + slot // SLOTS_CHUNK


def analysis_kernel(
    ny, nx, cells,
    model, driver, y_table, x_table, rate_in, cap_in, full, model_v,
    driver_v, rate, cap, y_v, x_v, weight, coef, from_y, row_sum, from_x,
    in_sem, table_sem, send_y, recv_y, send_x, recv_x,
    gather_x_send, gather_x_recv, gather_y_send, gather_y_recv, core_send, core_recv,
):
    fields, rows, columns = model.shape
    my_y, my_x = lax.axis_index("gy"), lax.axis_index("gx")
    pairs, steps = fields // 2, fields // FIELDS_STEP
    chunk_pairs = SLOTS_CHUNK * ny
    chunk_steps = chunk_pairs // 2
    chunks = nx // SLOTS_CHUNK

    def load(step):
        part = pl.ds(step * FIELDS_STEP, FIELDS_STEP)
        return (
            pltpu.make_async_copy(model.at[part], model_v.at[part], in_sem.at[step, 0]),
            pltpu.make_async_copy(driver.at[part], driver_v.at[part], in_sem.at[step, 1]),
        )

    table_copies = (
        pltpu.make_async_copy(y_table.at[my_y], y_v, table_sem.at[0]),
        pltpu.make_async_copy(x_table.at[my_x], x_v, table_sem.at[1]),
        pltpu.make_async_copy(rate_in, rate, table_sem.at[2]),
        pltpu.make_async_copy(cap_in, cap, table_sem.at[3]),
    )
    for copy in table_copies:
        copy.start()

    @pl.loop(0, steps)
    def _(step):
        for copy in load(step):
            copy.start()

    barrier = pltpu.get_barrier_semaphore()
    for k in range(1, ny):
        pl.semaphore_signal(
            barrier, inc=1, device_id=(lax.rem(my_y + k, ny), my_x), device_id_type=MESH
        )
    for k in range(1, nx):
        pl.semaphore_signal(
            barrier, inc=1, device_id=(my_y, lax.rem(my_x + k, nx)), device_id_type=MESH
        )

    for pair in range(pairs, ny * nx):
        coef[pair % ny, pair // ny] = jnp.zeros((KEPT, LANES), F32)
    for copy in table_copies:
        copy.wait()
    lane_w = lax.broadcasted_iota(jnp.int32, (columns, LANES), 1)
    for part, order in ((0, (0, 2)), (1, (1,))):
        value = x_v[part].astype(F32)
        left = jnp.where(lane_w < HALF, value, 0.0).astype(BF16)
        right = jnp.where(lane_w < HALF, 0.0, value).astype(BF16)
        for at in ((0, 1), (2,))[part]:
            weight[pl.ds(at * columns, columns)] = left
            weight[pl.ds((3 + at) * columns, columns)] = right

    lane = lax.broadcasted_iota(jnp.int32, (8, LANES), 1)

    def compute(step):
        for copy in load(step):
            copy.wait()
        sums, squares = [], []
        for pair in range(FIELDS_STEP // 2):
            blocks, marks = [], jnp.zeros((8, LANES), F32)
            for field in range(2):
                at = step * FIELDS_STEP + pair * 2 + field
                difference = driver_v[at] - model_v[at]
                high, low = split(difference)
                blocks += [high, low, high]
                part = jnp.sum((difference * difference).reshape(rows // 8, 8, columns), axis=0)
                mark = jnp.sum(part, axis=1, keepdims=True)
                marks = jnp.where(lane == field * HALF + KEPT, mark, marks)
            sums.append(dot(jnp.concatenate(blocks, axis=1), weight[...]))
            squares.append(marks)
        high, low = split(jnp.concatenate(sums, axis=1))
        first = dot(y_v[...], high)
        found = first[:KEPT] + first[KEPT:] + dot(y_v[:KEPT], low)
        for pair in range(FIELDS_STEP // 2):
            at = step * (FIELDS_STEP // 2) + pair
            g, q = lax.rem(at, ny), lax.div(at, ny)
            block = found[:, pair * LANES:(pair + 1) * LANES]
            coef[g, q, 0:8] = block[0:8] + squares[pair]
            coef[g, q, 8:KEPT] = block[8:]

    def to_rows(chunk, k):
        part = pl.ds(chunk * SLOTS_CHUNK, SLOTS_CHUNK)
        target = lax.rem(my_y + k, ny)
        return pltpu.make_async_remote_copy(
            src_ref=coef.at[target, part], dst_ref=from_y.at[k - 1, part],
            send_sem=send_y.at[chunk, k - 1], recv_sem=recv_y.at[chunk, k - 1],
            device_id=(target, my_x), device_id_type=MESH,
        )

    def to_owner(slot):
        target = owner_x(slot, nx)
        offset = lax.rem(my_x - target + nx, nx)
        return pltpu.make_async_remote_copy(
            src_ref=row_sum.at[slot], dst_ref=from_x.at[offset],
            send_sem=send_x.at[slot], recv_sem=recv_x.at[offset],
            device_id=(my_y, target), device_id_type=MESH,
        )

    def finish(chunk):
        for k in range(1, ny):
            to_rows(chunk, k).wait_recv()
        for slot in range(chunk * SLOTS_CHUNK, (chunk + 1) * SLOTS_CHUNK):
            total = coef[my_y, slot]
            for k in range(1, ny):
                total += from_y[k - 1, slot]
            row_sum[slot] = total

            @pl.when(my_x != owner_x(slot, nx))
            def _():
                to_owner(slot).start()

    for chunk in range(chunks):
        low, high = (min(steps, part * chunk_steps) for part in (chunk, chunk + 1))
        if high > low:
            pl.loop(low, high)(compute)
        if chunk == 0:
            pl.semaphore_wait(barrier, ny + nx - 2)
        for k in range(1, ny):
            to_rows(chunk, k).start()
        if chunk > 0:
            finish(chunk - 1)
    finish(chunks - 1)

    my_slot = lax.rem(my_x, nx // SLOTS_CHUNK) * SLOTS_CHUNK + lax.div(my_x, nx // SLOTS_CHUNK)
    my_pair = my_slot * ny + my_y
    total = row_sum[my_slot]
    for k in range(1, nx):
        pltpu.make_async_remote_copy(
            src_ref=row_sum.at[0], dst_ref=from_x.at[k],
            send_sem=send_x.at[0], recv_sem=recv_x.at[k],
            device_id=(my_y, lax.rem(my_x + k, nx)), device_id_type=MESH,
        ).wait_recv()
        total += from_x[k]
    lane_c = lax.broadcasted_iota(jnp.int32, (KEPT, LANES), 1)
    strength = []
    for field in range(2):
        at = jnp.minimum(my_pair * 2 + field, fields - 1)
        mark = jnp.where(lane_c == field * HALF + KEPT, total, 0.0)
        square = jnp.sum(jnp.sum(mark, axis=0, keepdims=True), axis=1, keepdims=True)
        spread = jnp.sqrt(square / cells + EPSILON)
        strength.append(rate[at] * jnp.minimum(1.0, cap[at] / spread))
    scale = jnp.where(lane_c < HALF, strength[0], strength[1])
    full[my_y, my_x] = jnp.where(lane_c % HALF < KEPT, total * scale, 0.0)

    half_y = ny // 2
    partner = my_y + 1 - 2 * lax.rem(my_y, 2)

    def x_of(k):
        return lax.rem(my_x - k + nx, nx)

    def y_of(j):
        return lax.rem(my_y - 2 * j + ny, ny)

    def gather_x(k):
        return pltpu.make_async_remote_copy(
            src_ref=full.at[my_y, my_x], dst_ref=full.at[my_y, my_x],
            send_sem=gather_x_send.at[k], recv_sem=gather_x_recv.at[k],
            device_id=(my_y, lax.rem(my_x + k, nx)), device_id_type=MESH,
        )

    def gather_y(j, k):
        return pltpu.make_async_remote_copy(
            src_ref=full.at[my_y, x_of(k)], dst_ref=full.at[my_y, x_of(k)],
            send_sem=gather_y_send.at[j, k], recv_sem=gather_y_recv.at[j, k],
            device_id=(lax.rem(my_y + 2 * j, ny), my_x), device_id_type=MESH,
        )

    def to_core(j, k):
        return pltpu.make_async_remote_copy(
            src_ref=full.at[y_of(j), x_of(k)], dst_ref=full.at[y_of(j), x_of(k)],
            send_sem=core_send.at[j, k], recv_sem=core_recv.at[j, k],
            device_id=(partner, my_x), device_id_type=MESH,
        )

    for k in range(1, nx):
        gather_x(k).start()
    for k in range(nx):
        if k:
            gather_x(k).wait_recv()
        for j in range(1, half_y):
            gather_y(j, k).start()
        to_core(0, k).start()
    for k in range(nx):
        for j in range(1, half_y):
            gather_y(j, k).wait_recv()
            to_core(j, k).start()
    for k in range(nx):
        for j in range(half_y):
            to_core(j, k).wait_recv()

    for chunk in range(chunks):
        for k in range(1, ny):
            to_rows(chunk, k).wait_send()
    for slot in range(nx):
        @pl.when(my_x != owner_x(slot, nx))
        def _():
            to_owner(slot).wait_send()
    for k in range(nx):
        if k:
            gather_x(k).wait_send()
        for j in range(half_y):
            if j:
                gather_y(j, k).wait_send()
            to_core(j, k).wait_send()


def build_kernel(ny, nx, model, full, y_table, x_table, out, y_v, x_v, weight, table_sem):
    step = pl.program_id(0)
    columns = model.shape[2]

    @pl.when(step == 0)
    def _():
        copies = (
            pltpu.make_async_copy(y_table.at[lax.axis_index("gy")], y_v, table_sem.at[0]),
            pltpu.make_async_copy(x_table.at[lax.axis_index("gx")], x_v, table_sem.at[1]),
        )
        for copy in copies:
            copy.start()
        for copy in copies:
            copy.wait()
        row = lax.broadcasted_iota(jnp.int32, (LANES, columns), 0)
        for part in range(2):
            value = x_v[part].astype(F32)
            left = jnp.where(row < HALF, value, 0.0).astype(BF16)
            right = jnp.where(row < HALF, 0.0, value).astype(BF16)
            both = jnp.concatenate([left, right], axis=1)
            for at in ((0, 1), (2,))[part]:
                weight[pl.ds(at * LANES, LANES)] = both

    for pair in range(BUILD_STEP // 2):
        at = step * (BUILD_STEP // 2) + pair
        high, low = split(full[lax.rem(at, ny), owner_x(lax.div(at, ny), nx)])
        along = dot(y_v[...], jnp.concatenate([high, low, high], axis=0))
        high, low = split(along)
        large = dot(jnp.concatenate([high, low, high], axis=1), weight[...])
        out[2 * pair] = model[2 * at] + large[:, :columns]
        out[2 * pair + 1] = model[2 * at + 1] + large[:, columns:]


def per_device(ny, nx, model, driver, rate, cap):
    fields, rows, columns = model.shape
    assert fields % FIELDS_STEP == fields % BUILD_STEP == 0 and fields // 2 <= ny * nx
    assert ny % 2 == 0 and nx % SLOTS_CHUNK == 0
    row_total, column_total = rows * ny, columns * nx
    y_in, x_in, y_out, x_out = (
        jnp.asarray(table) for table in tables(row_total, column_total, ny, nx)
    )
    anywhere = pl.BlockSpec(memory_space=pl.ANY)
    hbm = pl.BlockSpec(memory_space=pltpu.HBM)
    vector = pl.BlockSpec(memory_space=pltpu.VMEM)
    dma = pltpu.SemaphoreType.DMA
    chunks, half_y = nx // SLOTS_CHUNK, ny // 2
    kept = 4 * (fields * rows * columns + ny * nx * KEPT * LANES)
    room = VMEM_BYTES - kept - VMEM_SPARE
    full, model_kept = pl.pallas_call(
        functools.partial(analysis_kernel, ny, nx, float(row_total * column_total)),
        out_shape=(pltpu.VMEM((ny, nx, KEPT, LANES), F32), pltpu.VMEM(model.shape, F32)),
        in_specs=[hbm] * 6,
        out_specs=(vector, vector),
        scratch_shapes=[
            pltpu.VMEM((fields, rows, columns), F32),
            pltpu.SMEM((fields,), F32),
            pltpu.SMEM((fields,), F32),
            pltpu.VMEM((2 * KEPT, rows), BF16),
            pltpu.VMEM((2, columns, LANES), BF16),
            pltpu.VMEM((6 * columns, LANES), BF16),
            pltpu.VMEM((ny, nx, KEPT, LANES), F32),
            pltpu.VMEM((ny - 1, nx, KEPT, LANES), F32),
            pltpu.VMEM((nx, KEPT, LANES), F32),
            pltpu.VMEM((nx, KEPT, LANES), F32),
            dma((fields // FIELDS_STEP, 2)), dma((4,)),
            dma((chunks, ny - 1)), dma((chunks, ny - 1)), dma((nx,)), dma((nx,)),
            dma((nx,)), dma((nx,)), dma((half_y, nx)), dma((half_y, nx)),
            dma((half_y, nx)), dma((half_y, nx)),
        ],
        compiler_params=pltpu.CompilerParams(
            collective_id=0, has_side_effects=True, vmem_limit_bytes=room
        ),
        name="analysis",
    )(model, driver, y_in, x_in, rate, cap)
    block = pl.BlockSpec((BUILD_STEP, rows, columns), lambda i: (i, 0, 0))
    return pl.pallas_call(
        functools.partial(build_kernel, ny, nx),
        grid=(fields // BUILD_STEP,),
        out_shape=jax.ShapeDtypeStruct(model.shape, F32),
        in_specs=[vector, vector, anywhere, anywhere],
        out_specs=block,
        scratch_shapes=[
            pltpu.VMEM((rows, 3 * KEPT), BF16),
            pltpu.VMEM((2, LANES, columns), BF16),
            pltpu.VMEM((3 * LANES, 2 * columns), BF16),
            dma((2,)),
        ],
        compiler_params=pltpu.CompilerParams(
            dimension_semantics=("arbitrary",), vmem_limit_bytes=36 * 2**20
        ),
        name="build",
    )(model_kept, full, y_out, x_out)


def solution(mesh):
    return jax.shard_map(
        functools.partial(per_device, mesh.shape["gy"], mesh.shape["gx"]),
        mesh=mesh,
        in_specs=(P(None, "gy", "gx"), P(None, "gy", "gx"), P(), P()),
        out_specs=P(None, "gy", "gx"),
        check_vma=False,
    )
```
